32 devices in a mesh: gx: 4 (over y, x), gy: 4 (over z), gz: 2 (over core).
Axes of the slice: x: 2, y: 2, z: 4, core: 2. Of those that a mesh axis runs over, the one named last changes fastest.
Arguments:
- residual: float32 [2, 128, 128, 1024], P(None, 'gx', 'gy', 'gz'), may hold values from -6 to 6
- eig_x: float32 [4, 48, 48], P('gx'), may hold values from -0.875 to 0.875
- eig_y: float32 [4, 48, 48], P('gy'), may hold values from -0.875 to 0.875
- eig_z: float32 [2, 528, 528], P('gz'), may hold values from -0.25 to 0.25
- lam_x: float32 [4, 48], P('gx'), may hold values from 0.5 to 4
- lam_y: float32 [4, 48], P('gy'), may hold values from 0.5 to 4
- lam_z: float32 [2, 528], P('gz'), may hold values from 0.5 to 4
- basis_x: float32 [4, 4, 32], P('gx'), may hold values from -2.1 to 2.1
- basis_y: float32 [4, 4, 32], P('gy'), may hold values from -2.1 to 2.1
- basis_z: float32 [2, 4, 512], P('gz'), may hold values from -2.1 to 2.1
- coarse_inverse: float32 [2048, 2048], P(('gx', 'gy', 'gz')), may hold values from -0.0064086914 to 0.0064086914
Outputs:
- precond: float32 [2, 128, 128, 1024], P(None, 'gx', 'gy', 'gz')
The draws below stay inside these ranges and needn't reach their ends.
All inputs are finite; a program needn't handle non-finite values.
Results may differ from the reference program's by a relative error of at most 0.0003.
Values sent between devices are 32-bit elements; how exact they have to be, the bound alone decides.
A program may use at most 128 MiB of HBM per device.

```python
import math
import jax
import jax.numpy as jnp
from jax import lax

NODES = 8
CB = 4
NV = 2
MX = 32
MY = 32
MZ = 512
KX = 48
KY = 48
KZ = 528
NX = 128
NY = 128
NZ = 1024
NC = 2048
N_GX = 4
N_GY = 4
N_GZ = 2


def block_levels(stream_key, shape, split, low, top_value):
    def one(dim, blocks):
        steps = jax.random.uniform(jax.random.fold_in(jax.random.fold_in(stream_key, 6), dim), (blocks,), jnp.float32, low / len(split), top_value / len(split))
        return jnp.repeat(jnp.exp(steps), shape[dim] // blocks).reshape((-1,) + (1,) * (len(shape) - dim - 1))

    gain = one(*split[0])
    for cut in split[1:]:
        gain = gain * one(*cut)
    return gain


def noise(own_key, extent, width, most, shards=(), kind=jnp.bfloat16):
    entries = width * jax.random.normal(own_key, extent, jnp.float32)
    if shards:
        entries = entries * block_levels(own_key, extent, shards, -0.22, 0.18)
    return jnp.clip(entries, -most, most).astype(kind)


def setup_inputs(seed: int = 0) -> dict:
    key_of = jax.random.split(jax.random.key(seed), 12)
    residual = noise(key_of[0], (NV, NX, NY, NZ), 1.0, 6.0, ((1, 4), (2, 4), (3, 2)), jnp.float32)
    eig_x = noise(key_of[1], (N_GX, KX, KX), KX ** -0.5, 0.875, ((0, 4),), jnp.float32)
    eig_y = noise(key_of[2], (N_GY, KY, KY), KY ** -0.5, 0.875, ((0, 4),), jnp.float32)
    eig_z = noise(key_of[3], (N_GZ, KZ, KZ), KZ ** -0.5, 0.25, ((0, 2),), jnp.float32)
    lam_x = jnp.clip(jnp.exp(math.log(4.0) - 2.0794415 * jax.random.uniform(key_of[4], (N_GX, KX), jnp.float32) ** block_levels(key_of[4], (N_GX, KX), ((0, 4),), -0.2, 0.2)), 0.5, 4.0)
    lam_y = jnp.clip(jnp.exp(math.log(4.0) - 2.0794415 * jax.random.uniform(key_of[5], (N_GY, KY), jnp.float32) ** block_levels(key_of[5], (N_GY, KY), ((0, 4),), -0.2, 0.2)), 0.5, 4.0)
    lam_z = jnp.clip(jnp.exp(math.log(4.0) - 2.0794415 * jax.random.uniform(key_of[6], (N_GZ, KZ), jnp.float32) ** block_levels(key_of[6], (N_GZ, KZ), ((0, 2),), -0.2, 0.2)), 0.5, 4.0)
    basis_x = noise(key_of[7], (N_GX, CB, MX), 0.35, 2.1, ((0, 4),), jnp.float32)
    basis_y = noise(key_of[8], (N_GY, CB, MY), 0.35, 2.1, ((0, 4),), jnp.float32)
    basis_z = noise(key_of[9], (N_GZ, CB, MZ), 0.35, 2.1, ((0, 2),), jnp.float32)
    coarse_inverse = noise(key_of[10], (NC, NC), (35.0 / (MX * MY * MZ * NC) ** 0.5), 0.0064086914, ((0, 32),), jnp.float32)
    return {"residual": residual, "eig_x": eig_x, "eig_y": eig_y, "eig_z": eig_z, "lam_x": lam_x, "lam_y": lam_y, "lam_z": lam_z, "basis_x": basis_x, "basis_y": basis_y, "basis_z": basis_z, "coarse_inverse": coarse_inverse}


HIGH = lax.Precision.HIGHEST


def local_solve(ext, vec_x, vec_y, vec_z, val_x, val_y, val_z):
    spec = jnp.einsum('vabc,ai->vibc', ext, vec_x, precision=HIGH)
    spec = jnp.einsum('vibc,bj->vijc', spec, vec_y, precision=HIGH)
    spec = jnp.einsum('vijc,ck->vijk', spec, vec_z, precision=HIGH)
    spec = spec / (val_x[:, None, None] + val_y[None, :, None] + val_z[None, None, :])[None]
    back = jnp.einsum('vijk,ai->vajk', spec, vec_x, precision=HIGH)
    back = jnp.einsum('vajk,bj->vabk', back, vec_y, precision=HIGH)
    back = jnp.einsum('vabk,ck->vabc', back, vec_z, precision=HIGH)
    return back


def reference(residual, eig_x, eig_y, eig_z, lam_x, lam_y, lam_z, basis_x, basis_y, basis_z, coarse_inverse):
    padded = jnp.pad(residual, ((0, 0), (NODES, NODES), (NODES, NODES), (NODES, NODES)))

    def one_brick(linear):
        brick_i = (linear // (N_GY * N_GZ)).astype(jnp.int32)
        brick_j = ((linear // N_GZ) % N_GY).astype(jnp.int32)
        brick_k = (linear % N_GZ).astype(jnp.int32)
        zero = jnp.zeros((), jnp.int32)
        ext = lax.dynamic_slice(padded, (zero, brick_i * MX, brick_j * MY, brick_k * MZ), (NV, KX, KY, KZ))
        solved = local_solve(ext, eig_x[brick_i], eig_y[brick_j], eig_z[brick_k], lam_x[brick_i], lam_y[brick_j], lam_z[brick_k])
        return solved[:, NODES:NODES + MX, NODES:NODES + MY, NODES:NODES + MZ]

    stacked = lax.map(one_brick, jnp.arange(N_GX * N_GY * N_GZ, dtype=jnp.int32))
    stacked = stacked.reshape(N_GX, N_GY, N_GZ, NV, MX, MY, MZ)
    local = jnp.transpose(stacked, (3, 0, 4, 1, 5, 2, 6)).reshape(NV, NX, NY, NZ)

    field = residual.reshape(NV, N_GX, MX, N_GY, MY, N_GZ, MZ)
    part = jnp.einsum('viajbkc,ipa->vipjbkc', field, basis_x, precision=HIGH)
    part = jnp.einsum('vipjbkc,jqb->vipjqkc', part, basis_y, precision=HIGH)
    coarse = jnp.einsum('vipjqkc,ksc->ijkpqsv', part, basis_z, precision=HIGH).reshape(NC, NV)
    coarse_sol = jnp.dot(coarse_inverse, coarse, precision=HIGH)
    blocks = coarse_sol.reshape(N_GX, N_GY, N_GZ, CB, CB, CB, NV)
    spread = jnp.einsum('ijkpqsv,ksc->ijpqvkc', blocks, basis_z, precision=HIGH)
    spread = jnp.einsum('ijpqvkc,jqb->ipvjbkc', spread, basis_y, precision=HIGH)
    spread = jnp.einsum('ipvjbkc,ipa->viajbkc', spread, basis_x, precision=HIGH).reshape(NV, NX, NY, NZ)
    return local + spread
```

```python
import functools

import jax
import jax.numpy as jnp
from jax import lax
from jax.experimental import pallas as pl
from jax.experimental.pallas import tpu as pltpu
from jax.sharding import PartitionSpec as P

NODES = 8
LANES = 128
HIGH = lax.Precision.HIGHEST
BF = jnp.bfloat16
F32 = jnp.float32


def split_host(x):
    hi = lax.reduce_precision(x, 8, 7)
    return hi.astype(BF), lax.reduce_precision(x - hi, 8, 7).astype(BF)


def split(x):
    hi = x.astype(BF)
    return hi, (x - hi.astype(F32)).astype(BF)


def halo_kernel(
    sizes, res, bz, kron, ext, every, zeros, part, own_sem, zero_sem, sx, rx, sy, ry, sc, rc, sg, rg
):
    n_gx, n_gy, n_gz = sizes
    own_x, own_y = res.shape[1], res.shape[2]
    w = NODES
    gx = lax.axis_index("gx")
    gy = lax.axis_index("gy")
    has_x = (gx > 0, gx < n_gx - 1)
    has_y = (gy > 0, gy < n_gy - 1)
    to_x = (gx - 1, gx + 1)
    to_y = (gy - 1, gy + 1)
    gz = lax.axis_index("gz")
    place = {"gx": gx, "gy": gy, "gz": gz}
    barrier = pltpu.get_barrier_semaphore()
    peers = [
        {axis: lax.rem(place[axis] + step, count)}
        for axis, count in zip(("gz", "gy", "gx"), (n_gz, n_gy, n_gx))
        for step in range(1, count)
    ]
    for peer in peers:
        pl.semaphore_signal(barrier, inc=1, device_id=peer)
    pl.semaphore_wait(barrier, len(peers))

    src = lambda side, own: pl.ds(0, w) if side == 0 else pl.ds(own - w, w)
    dst = lambda side, own: pl.ds(own + w, w) if side == 0 else pl.ds(0, w)
    mine = lambda side, own: pl.ds(0, w) if side == 0 else pl.ds(own + w, w)
    chunks = ((0, w), (own_y - w, w), (w, own_y - 2 * w))

    def send_x(side, c):
        start, size = chunks[c]
        return pltpu.make_async_remote_copy(
            src_ref=res.at[:, src(side, own_x), pl.ds(start, size)],
            dst_ref=ext.at[:, dst(side, own_x), pl.ds(w + start, size)],
            send_sem=sx.at[side, c],
            recv_sem=rx.at[side, c],
            device_id={"gx": to_x[side]},
        )

    def get_x(side, c):
        start, size = chunks[c]
        return pltpu.make_async_remote_copy(
            src_ref=res.at[:, src(1 - side, own_x), pl.ds(start, size)],
            dst_ref=ext.at[:, mine(side, own_x), pl.ds(w + start, size)],
            send_sem=sx.at[1 - side, c],
            recv_sem=rx.at[1 - side, c],
            device_id={"gx": to_x[side]},
        )

    def send_y(side):
        return pltpu.make_async_remote_copy(
            src_ref=res.at[:, :, src(side, own_y)],
            dst_ref=ext.at[:, pl.ds(w, own_x), dst(side, own_y)],
            send_sem=sy.at[side],
            recv_sem=ry.at[side],
            device_id={"gy": to_y[side]},
        )

    def get_y(side):
        return pltpu.make_async_remote_copy(
            src_ref=res.at[:, :, src(1 - side, own_y)],
            dst_ref=ext.at[:, pl.ds(w, own_x), mine(side, own_y)],
            send_sem=sy.at[1 - side],
            recv_sem=ry.at[1 - side],
            device_id={"gy": to_y[side]},
        )

    def send_c(a, b):
        rows = pl.ds(w, w) if b == 0 else pl.ds(own_y, w)
        return pltpu.make_async_remote_copy(
            src_ref=ext.at[:, mine(a, own_x), rows],
            dst_ref=ext.at[:, mine(a, own_x), dst(b, own_y)],
            send_sem=sc.at[a, b],
            recv_sem=rc.at[a, b],
            device_id={"gy": to_y[b]},
        )

    def get_c(a, b):
        return pltpu.make_async_remote_copy(
            src_ref=ext.at[:, mine(a, own_x), pl.ds(w, w)],
            dst_ref=ext.at[:, mine(a, own_x), mine(b, own_y)],
            send_sem=sc.at[a, 1 - b],
            recv_sem=rc.at[a, 1 - b],
            device_id={"gy": to_y[b]},
        )

    for c in range(3):
        for side in range(2):
            @pl.when(has_x[side])
            def _():
                send_x(side, c).start()

    own = pltpu.make_async_copy(
        res, ext.at[:, pl.ds(w, own_x), pl.ds(w, own_y)], own_sem
    )
    own.start()
    zeros[...] = jnp.zeros_like(zeros)

    nv, mz = res.shape[0], res.shape[3]
    rows, lanes = part.shape[1], part.shape[2]
    step = 4

    @pl.loop(0, nv * (own_x // step))
    def _(i):
        v = i // (own_x // step)
        a = lax.rem(i, own_x // step)
        hi, lo = split(res[v, pl.ds(a * step, step)].reshape(step * own_y, mz))
        both = dot(hi, bz[...])
        both = both[:, :lanes] + both[:, lanes:] + dot(lo, bz[:, :lanes])
        part[v, pl.ds(pl.multiple_of(a * (step * own_y), 8), step * own_y), :] = both

    pairs = kron.shape[0]
    funcs = lanes // (nv * pairs)
    lane = lax.broadcasted_iota(jnp.int32, (pairs, lanes), 1)
    row = lax.broadcasted_iota(jnp.int32, (pairs, lanes), 0)
    total = jnp.zeros((1, lanes), F32)
    for v in range(nv):
        full = dot(kron[...], stack3(part[v]))
        keep = lane - row * funcs - v * (pairs * funcs)
        keep = jnp.logical_and(keep >= 0, keep < funcs)
        total += jnp.sum(jnp.where(keep, full, 0.0), axis=0, keepdims=True)
    every[gx, gy, gz] = total

    def stage(level):
        axis, count = (("gz", n_gz), ("gy", n_gy), ("gx", n_gx))[level]
        at = (every.at[gx, gy, gz], every.at[gx, gy], every.at[gx])[level]
        return [
            pltpu.make_async_remote_copy(
                src_ref=at, dst_ref=at, send_sem=sg.at[level, k - 1], recv_sem=rg.at[level, k - 1],
                device_id={axis: lax.rem(place[axis] + k, count)})
            for k in range(1, count)
        ]

    def arrived(level):
        axis, count = (("gz", n_gz), ("gy", n_gy), ("gx", n_gx))[level]
        for k in range(1, count):
            who = lax.rem(place[axis] + count - k, count)
            at = (every.at[gx, gy, who], every.at[gx, who], every.at[who])[level]
            pltpu.make_async_remote_copy(
                src_ref=at, dst_ref=at, send_sem=sg.at[level, k - 1], recv_sem=rg.at[level, k - 1],
                device_id={axis: who}).wait_recv()

    for copy in stage(0):
        copy.start()
    arrived(0)
    for copy in stage(1):
        copy.start()
    for side in range(2):
        @pl.when(has_y[side])
        def _():
            send_y(side).start()
    arrived(1)
    for copy in stage(2):
        copy.start()

    def zero_x(side):
        return pltpu.make_async_copy(
            zeros.at[:, pl.ds(0, w)],
            ext.at[:, mine(side, own_x), pl.ds(w, own_y)], zero_sem.at[side])

    def zero_y(side):
        return pltpu.make_async_copy(
            zeros.at[:, pl.ds(0, own_x), pl.ds(0, w)],
            ext.at[:, pl.ds(w, own_x), mine(side, own_y)], zero_sem.at[2 + side])

    def zero_c(a, b):
        return pltpu.make_async_copy(
            zeros.at[:, pl.ds(0, w), pl.ds(0, w)],
            ext.at[:, mine(a, own_x), mine(b, own_y)], zero_sem.at[4 + 2 * a + b])

    both = lambda a, b: jnp.logical_and(has_x[a], has_y[b])
    for s in range(2):
        pl.when(jnp.logical_not(has_x[s]))(lambda: zero_x(s).start())
        pl.when(jnp.logical_not(has_y[s]))(lambda: zero_y(s).start())
        for b in range(2):
            pl.when(jnp.logical_not(both(s, b)))(lambda: zero_c(s, b).start())

    for c in range(2):
        for a in range(2):
            @pl.when(has_x[a])
            def _():
                get_x(a, c).wait_recv()

            @pl.when(both(a, c))
            def _():
                send_c(a, c).start()
    for a in range(2):
        pl.when(has_x[a])(lambda: get_x(a, 2).wait_recv())
        pl.when(has_y[a])(lambda: get_y(a).wait_recv())
        for b in range(2):
            pl.when(both(a, b))(lambda: get_c(a, b).wait_recv())
    arrived(2)
    for level in range(3):
        for copy in stage(level):
            copy.wait_send()
    own.wait()
    for s in range(2):
        pl.when(jnp.logical_not(has_x[s]))(lambda: zero_x(s).wait())
        pl.when(jnp.logical_not(has_y[s]))(lambda: zero_y(s).wait())
        for b in range(2):
            pl.when(jnp.logical_not(both(s, b)))(lambda: zero_c(s, b).wait())
            pl.when(both(s, b))(lambda: send_c(s, b).wait_send())
        for c in range(3):
            pl.when(has_x[s])(lambda: send_x(s, c).wait_send())
        pl.when(has_y[s])(lambda: send_y(s).wait_send())


def extend(residual, bz, kron):
    sizes = tuple(lax.axis_size(axis) for axis in ("gx", "gy", "gz"))
    lanes = bz.shape[1] // 2
    peers = max(max(sizes) - 1, 1)
    nv, mx, my, mz = residual.shape
    w = NODES
    return pl.pallas_call(
        functools.partial(halo_kernel, sizes),
        out_shape=(
            jax.ShapeDtypeStruct((nv, mx + 2 * w, my + 2 * w, mz), F32),
            jax.ShapeDtypeStruct(sizes + (1, lanes), F32),
        ),
        in_specs=[pl.BlockSpec(memory_space=pltpu.VMEM)] * 3,
        out_specs=(
            pl.BlockSpec(memory_space=pltpu.HBM),
            pl.BlockSpec(memory_space=pltpu.VMEM),
        ),
        scratch_shapes=[
            pltpu.VMEM((nv, max(w, mx), my, mz), F32),
            pltpu.VMEM((nv, mx * my, lanes), F32),
            pltpu.SemaphoreType.DMA,
            pltpu.SemaphoreType.DMA((8,)),
            pltpu.SemaphoreType.DMA((2, 3)),
            pltpu.SemaphoreType.DMA((2, 3)),
            pltpu.SemaphoreType.DMA((2,)),
            pltpu.SemaphoreType.DMA((2,)),
            pltpu.SemaphoreType.DMA((2, 2)),
            pltpu.SemaphoreType.DMA((2, 2)),
            pltpu.SemaphoreType.DMA((3, peers)),
            pltpu.SemaphoreType.DMA((3, peers)),
        ],
        compiler_params=pltpu.CompilerParams(
            collective_id=0, has_side_effects=True, vmem_limit_bytes=32 * 2**20),
        name="halo",
    )(residual, bz, kron)


def stack3(x):
    hi, lo = split(x)
    return jnp.concatenate([hi, lo, hi], axis=0)


def dot(a, b):
    return jnp.dot(a, b, preferred_element_type=F32)


def load_rows(refs, start, size, stride):
    return jnp.concatenate([ref[pl.ds(start, size, stride), :] for ref in refs], axis=1)


def store_rows(refs, start, size, value):
    for i, ref in enumerate(refs):
        ref[pl.ds(pl.multiple_of(start, 8), size), :] = value[:, i * LANES : (i + 1) * LANES]


def forward_kernel(kx, ky, left, right, ex, ey, out, *tmp):
    ext = (left.at[0], right.at[0])

    @pl.loop(0, ky, unroll=8)
    def _(y):
        part = dot(ex[...], stack3(load_rows(ext, y, kx, ky)))
        store_rows(tmp, y * kx, kx, part)

    @pl.loop(0, kx, unroll=8)
    def _(p):
        part = dot(ey[...], stack3(load_rows(tmp, p, ky, kx)))
        out[0, pl.ds(pl.multiple_of(p * ky, 8), ky), :] = part


def forward_xy(ext, ex3, ey3, kx, ky):
    nv, rows, mz = ext.shape
    wide = 2 * LANES
    return pl.pallas_call(
        functools.partial(forward_kernel, kx, ky),
        grid=(nv, mz // wide),
        out_shape=jax.ShapeDtypeStruct(ext.shape, F32),
        in_specs=[
            pl.BlockSpec((1, rows, LANES), lambda v, z: (v, 0, 2 * z)),
            pl.BlockSpec((1, rows, LANES), lambda v, z: (v, 0, 2 * z + 1)),
            pl.BlockSpec(memory_space=pltpu.VMEM),
            pl.BlockSpec(memory_space=pltpu.VMEM),
        ],
        out_specs=pl.BlockSpec((1, rows, wide), lambda v, z: (v, 0, z)),
        scratch_shapes=[pltpu.VMEM((rows, LANES), F32)] * 2,
        compiler_params=pltpu.CompilerParams(vmem_limit_bytes=32 * 2**20),
        name="forward_xy",
    )(ext, ext, ex3, ey3)


def z_kernel(mz, t, low, high, lxy, lz, w1, w2, out):
    w = NODES
    lane = lax.broadcasted_iota(jnp.int32, low.shape, 1)
    edge = jnp.where(lane < w, high[...], jnp.where(lane >= LANES - w, low[...], 0.0))

    def pack(x):
        hi = x.astype(BF).astype(F32)
        lo = x - hi
        return (hi + pltpu.roll(lo, 2 * w, 1) + pltpu.roll(hi, 4 * w, 1)).astype(BF)

    hi, lo = split(t[...])
    spec = dot(jnp.concatenate([hi, lo, hi, pack(edge)], axis=1), w1[...])
    spec = spec / (lxy[:, :1] + lz[...])
    hi, lo = split(spec[:, :mz])
    out[...] = dot(jnp.concatenate([hi, lo, hi, pack(spec[:, mz:])], axis=1), w2[...])


def solve_z(t, low, high, lxy, lz, w1, w2):
    rows, mz = t.shape
    r = 288
    per = lxy.shape[0] // r
    row = lambda i: (i, 0)
    return pl.pallas_call(
        functools.partial(z_kernel, mz),
        grid=(rows // r,),
        out_shape=jax.ShapeDtypeStruct(t.shape, F32),
        in_specs=[
            pl.BlockSpec((r, mz), row),
            pl.BlockSpec((r, LANES), row),
            pl.BlockSpec((r, LANES), row),
            pl.BlockSpec((r, LANES), lambda i: (lax.rem(i, per), 0)),
            pl.BlockSpec(memory_space=pltpu.VMEM),
            pl.BlockSpec(memory_space=pltpu.VMEM),
            pl.BlockSpec(memory_space=pltpu.VMEM),
        ],
        out_specs=pl.BlockSpec((r, mz), row),
        compiler_params=pltpu.CompilerParams(vmem_limit_bytes=40 * 2**20),
        name="solve_z",
    )(t, low, high, lxy, lz, w1, w2)


def backward_kernel(kx, ky, mx, my, left, right, c3, ex, ey, out, *tmp):
    u = (left.at[0], right.at[0])

    @pl.loop(0, ky, unroll=8)
    def _(q):
        part = dot(ex[...], stack3(load_rows(u, q, kx, ky)))
        store_rows(tmp, q * mx, mx, part)

    @pl.loop(0, mx, unroll=8)
    def _(a):
        slab = stack3(load_rows(tmp, a, ky, mx))
        slab = jnp.concatenate([slab, c3[0, a]], axis=0)
        out[0, pl.ds(pl.multiple_of(a * my, 8), my), :] = dot(ey[...], slab)


def backward_xy(u, c3, ex3, ey3, kx, ky, mx, my):
    nv, rows, mz = u.shape
    wide = 2 * LANES
    return pl.pallas_call(
        functools.partial(backward_kernel, kx, ky, mx, my),
        grid=(nv, mz // wide),
        out_shape=jax.ShapeDtypeStruct((nv, mx * my, mz), F32),
        in_specs=[
            pl.BlockSpec((1, rows, LANES), lambda v, z: (v, 0, 2 * z)),
            pl.BlockSpec((1, rows, LANES), lambda v, z: (v, 0, 2 * z + 1)),
            pl.BlockSpec((1,) + c3.shape[1:3] + (wide,), lambda v, z: (v, 0, 0, z)),
            pl.BlockSpec(memory_space=pltpu.VMEM),
            pl.BlockSpec(memory_space=pltpu.VMEM),
        ],
        out_specs=pl.BlockSpec((1, mx * my, wide), lambda v, z: (v, 0, z)),
        scratch_shapes=[pltpu.VMEM((ky * mx, LANES), F32)] * 2,
        compiler_params=pltpu.CompilerParams(vmem_limit_bytes=32 * 2**20),
        name="backward_xy",
    )(u, u, c3, ex3, ey3)


def left3(m):
    hi, lo = split_host(m)
    return jnp.concatenate([hi, hi, lo], axis=1)


def shifted(x, axis, step):
    count = lax.axis_size(axis)
    pairs = [(i, i + step) for i in range(count) if 0 <= i + step < count]
    return lax.ppermute(x, axis, pairs)


def body(
    residual, eig_x, eig_y, eig_z, lam_x, lam_y, lam_z, basis_x, basis_y, basis_z, coarse_inverse
):
    w = NODES
    nv, mx, my, mz = residual.shape
    kx, ky, kz = eig_x.shape[1], eig_y.shape[1], eig_z.shape[1]
    funcs = basis_x.shape[1]
    bx, by, bz = basis_x[0], basis_y[0], basis_z[0]

    block = funcs**3
    bh, bl = split_host(jnp.tile(bz.T, (1, nv * funcs * funcs)))
    kron = (bx[:, None, :, None] * by[None, :, None, :]).reshape(funcs * funcs, mx * my)
    ext, every = extend(residual, jnp.concatenate([bh, bl], axis=1), left3(kron))
    ext = ext.reshape(nv, kx * ky, mz)

    coarse = jnp.swapaxes(every.reshape(-1, nv, block), 1, 2).reshape(-1, nv)
    sol = jnp.dot(coarse_inverse, coarse, precision=HIGH).T.reshape(nv, funcs, funcs, funcs)
    wide = jnp.einsum("vpqs,pa->vaqs", sol, bx, precision=HIGH)
    wide = jnp.einsum("vaqs,sc->vaqc", wide, bz, precision=HIGH)
    hi, lo = split_host(wide)
    pad = -(3 * funcs) % 16
    c3 = jnp.concatenate([hi, lo, hi, jnp.zeros((nv, mx, pad, mz), BF)], axis=2)

    ex, ey, ez = eig_x[0], eig_y[0], eig_z[0]
    t = forward_xy(ext, left3(ex.T), left3(ey.T), kx, ky)
    edge = jnp.concatenate(
        [t[:, :, : LANES // 2], t[:, :, mz - LANES // 2 :]], axis=2).reshape(-1, LANES)
    low, high = shifted(edge, "gz", 1), shifted(edge, "gz", -1)

    extra = LANES - (kz - mz)
    eh, el = split_host(jnp.pad(ez, ((0, 0), (0, extra))))
    gap = jnp.zeros((LANES - 7 * w, mz + LANES), BF)
    top, end = slice(0, w), slice(kz - w, kz)
    w1 = jnp.concatenate(
        [eh[w : w + mz], eh[w : w + mz], el[w : w + mz],
         eh[end], eh[top], eh[end], el[top], el[end], gap, jnp.zeros((w, mz + LANES), BF), eh[top]], axis=0)
    bh, bl = split_host(ez[w : w + mz].T)
    gap = jnp.zeros((LANES - 3 * (kz - mz), mz), BF)
    w2 = jnp.concatenate([bh[:mz], bh[:mz], bl[:mz], bh[mz:], bh[mz:], bl[mz:], gap], axis=0)
    lxy = jnp.broadcast_to(
        (lam_x[0][:, None] + lam_y[0][None, :]).reshape(kx * ky, 1), (kx * ky, LANES))
    lz = jnp.pad(lam_z[0], (0, extra), constant_values=1.0)[None]
    u = solve_z(t.reshape(nv * kx * ky, mz), low, high, lxy, lz, w1, w2)

    bh, bl = split_host(by.T)
    ey3 = jnp.concatenate(
        [left3(ey[w : w + my]), bh, bh, bl, jnp.zeros((my, pad), BF)], axis=1)
    out = backward_xy(
        u.reshape(nv, kx * ky, mz), c3, left3(ex[w : w + mx]), ey3, kx, ky, mx, my)
    return out.reshape(nv, mx, my, mz)


def solution(mesh):
    in_specs = (
        P(None, "gx", "gy", "gz"),
        P("gx", None, None),
        P("gy", None, None),
        P("gz", None, None),
        P("gx", None),
        P("gy", None),
        P("gz", None),
        P("gx", None, None),
        P("gy", None, None),
        P("gz", None, None),
        P(("gx", "gy", "gz"), None),
    )
    out_specs = P(None, "gx", "gy", "gz")
    return jax.shard_map(body, mesh=mesh, in_specs=in_specs, out_specs=out_specs, check_vma=False)
```

```python
import functools

import jax
import jax.numpy as jnp
from jax import lax
from jax.experimental import pallas as pl
from jax.experimental.pallas import tpu as pltpu
from jax.sharding import PartitionSpec as P

NODES = 8
LANES = 128
HIGH = lax.Precision.HIGHEST
BF = jnp.bfloat16
F32 = jnp.float32


def split_host(x):
    hi = lax.reduce_precision(x, 8, 7)
    return hi.astype(BF), lax.reduce_precision(x - hi, 8, 7).astype(BF)


def split(x):
    hi = x.astype(BF)
    return hi, (x - hi.astype(F32)).astype(BF)


def halo_kernel(
    sizes, res, bz, kron, ext, every, zeros, part, own_sem, zero_sem, sx, rx, sy, ry, sc, rc, sg, rg
):
    n_gx, n_gy, n_gz = sizes
    own_x, own_y = res.shape[1], res.shape[2]
    w = NODES
    gx = lax.axis_index("gx")
    gy = lax.axis_index("gy")
    has_x = (gx > 0, gx < n_gx - 1)
    has_y = (gy > 0, gy < n_gy - 1)
    to_x = (gx - 1, gx + 1)
    to_y = (gy - 1, gy + 1)
    gz = lax.axis_index("gz")
    place = {"gx": gx, "gy": gy, "gz": gz}
    barrier = pltpu.get_barrier_semaphore()
    peers = [
        {axis: lax.rem(place[axis] + step, count)}
        for axis, count in zip(("gz", "gy", "gx"), (n_gz, n_gy, n_gx))
        for step in range(1, count)
    ]
    for peer in peers:
        pl.semaphore_signal(barrier, inc=1, device_id=peer)
    pl.semaphore_wait(barrier, len(peers))

    src = lambda side, own: pl.ds(0, w) if side == 0 else pl.ds(own - w, w)
    dst = lambda side, own: pl.ds(own + w, w) if side == 0 else pl.ds(0, w)
    mine = lambda side, own: pl.ds(0, w) if side == 0 else pl.ds(own + w, w)
    chunks = ((0, w), (own_y - w, w), (w, own_y - 2 * w))

    def send_x(side, c):
        start, size = chunks[c]
        return pltpu.make_async_remote_copy(
            src_ref=res.at[:, src(side, own_x), pl.ds(start, size)],
            dst_ref=ext.at[:, dst(side, own_x), pl.ds(w + start, size)],
            send_sem=sx.at[side, c],
            recv_sem=rx.at[side, c],
            device_id={"gx": to_x[side]},
        )

    def get_x(side, c):
        start, size = chunks[c]
        return pltpu.make_async_remote_copy(
            src_ref=res.at[:, src(1 - side, own_x), pl.ds(start, size)],
            dst_ref=ext.at[:, mine(side, own_x), pl.ds(w + start, size)],
            send_sem=sx.at[1 - side, c],
            recv_sem=rx.at[1 - side, c],
            device_id={"gx": to_x[side]},
        )

    def send_y(side):
        return pltpu.make_async_remote_copy(
            src_ref=res.at[:, :, src(side, own_y)],
            dst_ref=ext.at[:, pl.ds(w, own_x), dst(side, own_y)],
            send_sem=sy.at[side],
            recv_sem=ry.at[side],
            device_id={"gy": to_y[side]},
        )

    def get_y(side):
        return pltpu.make_async_remote_copy(
            src_ref=res.at[:, :, src(1 - side, own_y)],
            dst_ref=ext.at[:, pl.ds(w, own_x), mine(side, own_y)],
            send_sem=sy.at[1 - side],
            recv_sem=ry.at[1 - side],
            device_id={"gy": to_y[side]},
        )

    def send_c(a, b):
        rows = pl.ds(w, w) if b == 0 else pl.ds(own_y, w)
        return pltpu.make_async_remote_copy(
            src_ref=ext.at[:, mine(a, own_x), rows],
            dst_ref=ext.at[:, mine(a, own_x), dst(b, own_y)],
            send_sem=sc.at[a, b],
            recv_sem=rc.at[a, b],
            device_id={"gy": to_y[b]},
        )

    def get_c(a, b):
        return pltpu.make_async_remote_copy(
            src_ref=ext.at[:, mine(a, own_x), pl.ds(w, w)],
            dst_ref=ext.at[:, mine(a, own_x), mine(b, own_y)],
            send_sem=sc.at[a, 1 - b],
            recv_sem=rc.at[a, 1 - b],
            device_id={"gy": to_y[b]},
        )

    for c in range(3):
        for side in range(2):
            @pl.when(has_x[side])
            def _():
                send_x(side, c).start()

    for side in range(2):
        @pl.when(has_y[side])
        def _():
            send_y(side).start()

    own = pltpu.make_async_copy(
        res, ext.at[:, pl.ds(w, own_x), pl.ds(w, own_y)], own_sem
    )
    own.start()
    zeros[...] = jnp.zeros_like(zeros)

    nv, mz = res.shape[0], res.shape[3]
    rows, lanes = part.shape[1], part.shape[2]
    step = 4

    @pl.loop(0, nv * (own_x // step))
    def _(i):
        v = i // (own_x // step)
        a = lax.rem(i, own_x // step)
        hi, lo = split(res[v, pl.ds(a * step, step)].reshape(step * own_y, mz))
        both = dot(hi, bz[...])
        both = both[:, :lanes] + both[:, lanes:] + dot(lo, bz[:, :lanes])
        part[v, pl.ds(pl.multiple_of(a * (step * own_y), 8), step * own_y), :] = both

    pairs = kron.shape[0]
    funcs = lanes // (nv * pairs)
    lane = lax.broadcasted_iota(jnp.int32, (pairs, lanes), 1)
    row = lax.broadcasted_iota(jnp.int32, (pairs, lanes), 0)
    total = jnp.zeros((1, lanes), F32)
    for v in range(nv):
        full = dot(kron[...], stack3(part[v]))
        keep = lane - row * funcs - v * (pairs * funcs)
        keep = jnp.logical_and(keep >= 0, keep < funcs)
        total += jnp.sum(jnp.where(keep, full, 0.0), axis=0, keepdims=True)
    every[gx, gy, gz] = total

    def stage(level):
        axis, count = (("gz", n_gz), ("gy", n_gy), ("gx", n_gx))[level]
        at = (every.at[gx, gy, gz], every.at[gx, gy], every.at[gx])[level]
        return [
            pltpu.make_async_remote_copy(
                src_ref=at, dst_ref=at, send_sem=sg.at[level, k - 1], recv_sem=rg.at[level, k - 1],
                device_id={axis: lax.rem(place[axis] + k, count)})
            for k in range(1, count)
        ]

    def arrived(level):
        axis, count = (("gz", n_gz), ("gy", n_gy), ("gx", n_gx))[level]
        for k in range(1, count):
            who = lax.rem(place[axis] + count - k, count)
            at = (every.at[gx, gy, who], every.at[gx, who], every.at[who])[level]
            pltpu.make_async_remote_copy(
                src_ref=at, dst_ref=at, send_sem=sg.at[level, k - 1], recv_sem=rg.at[level, k - 1],
                device_id={axis: who}).wait_recv()

    for copy in stage(0):
        copy.start()
    arrived(0)
    for copy in stage(1):
        copy.start()
    def zero_x(side):
        return pltpu.make_async_copy(
            zeros.at[:, pl.ds(0, w)],
            ext.at[:, mine(side, own_x), pl.ds(w, own_y)], zero_sem.at[side])

    def zero_y(side):
        return pltpu.make_async_copy(
            zeros.at[:, pl.ds(0, own_x), pl.ds(0, w)],
            ext.at[:, pl.ds(w, own_x), mine(side, own_y)], zero_sem.at[2 + side])

    def zero_c(a, b):
        return pltpu.make_async_copy(
            zeros.at[:, pl.ds(0, w), pl.ds(0, w)],
            ext.at[:, mine(a, own_x), mine(b, own_y)], zero_sem.at[4 + 2 * a + b])

    both = lambda a, b: jnp.logical_and(has_x[a], has_y[b])
    for s in range(2):
        pl.when(jnp.logical_not(has_x[s]))(lambda: zero_x(s).start())
        pl.when(jnp.logical_not(has_y[s]))(lambda: zero_y(s).start())
        for b in range(2):
            pl.when(jnp.logical_not(both(s, b)))(lambda: zero_c(s, b).start())

    for c in range(2):
        for a in range(2):
            @pl.when(has_x[a])
            def _():
                get_x(a, c).wait_recv()

            @pl.when(both(a, c))
            def _():
                send_c(a, c).start()
    arrived(1)
    for copy in stage(2):
        copy.start()
    for a in range(2):
        pl.when(has_x[a])(lambda: get_x(a, 2).wait_recv())
        pl.when(has_y[a])(lambda: get_y(a).wait_recv())
        for b in range(2):
            pl.when(both(a, b))(lambda: get_c(a, b).wait_recv())
    arrived(2)
    for level in range(3):
        for copy in stage(level):
            copy.wait_send()
    own.wait()
    for s in range(2):
        pl.when(jnp.logical_not(has_x[s]))(lambda: zero_x(s).wait())
        pl.when(jnp.logical_not(has_y[s]))(lambda: zero_y(s).wait())
        for b in range(2):
            pl.when(jnp.logical_not(both(s, b)))(lambda: zero_c(s, b).wait())
            pl.when(both(s, b))(lambda: send_c(s, b).wait_send())
        for c in range(3):
            pl.when(has_x[s])(lambda: send_x(s, c).wait_send())
        pl.when(has_y[s])(lambda: send_y(s).wait_send())


def extend(residual, bz, kron):
    sizes = tuple(lax.axis_size(axis) for axis in ("gx", "gy", "gz"))
    lanes = bz.shape[1] // 2
    peers = max(max(sizes) - 1, 1)
    nv, mx, my, mz = residual.shape
    w = NODES
    return pl.pallas_call(
        functools.partial(halo_kernel, sizes),
        out_shape=(
            jax.ShapeDtypeStruct((nv, mx + 2 * w, my + 2 * w, mz), F32),
            jax.ShapeDtypeStruct(sizes + (1, lanes), F32),
        ),
        in_specs=[pl.BlockSpec(memory_space=pltpu.VMEM)] * 3,
        out_specs=(
            pl.BlockSpec(memory_space=pltpu.HBM),
            pl.BlockSpec(memory_space=pltpu.VMEM),
        ),
        scratch_shapes=[
            pltpu.VMEM((nv, max(w, mx), my, mz), F32),
            pltpu.VMEM((nv, mx * my, lanes), F32),
            pltpu.SemaphoreType.DMA,
            pltpu.SemaphoreType.DMA((8,)),
            pltpu.SemaphoreType.DMA((2, 3)),
            pltpu.SemaphoreType.DMA((2, 3)),
            pltpu.SemaphoreType.DMA((2,)),
            pltpu.SemaphoreType.DMA((2,)),
            pltpu.SemaphoreType.DMA((2, 2)),
            pltpu.SemaphoreType.DMA((2, 2)),
            pltpu.SemaphoreType.DMA((3, peers)),
            pltpu.SemaphoreType.DMA((3, peers)),
        ],
        compiler_params=pltpu.CompilerParams(
            collective_id=0, has_side_effects=True, vmem_limit_bytes=56 * 2**20),
        name="halo",
    )(residual, bz, kron)


def stack3(x):
    hi, lo = split(x)
    return jnp.concatenate([hi, lo, hi], axis=0)


def dot(a, b):
    return jnp.dot(a, b, preferred_element_type=F32)


def load_rows(refs, start, size, stride):
    return jnp.concatenate([ref[pl.ds(start, size, stride), :] for ref in refs], axis=1)


def store_rows(refs, start, size, value):
    for i, ref in enumerate(refs):
        ref[pl.ds(pl.multiple_of(start, 8), size), :] = value[:, i * LANES : (i + 1) * LANES]


def forward_kernel(kx, ky, left, right, ex, ey, out, edge, *tmp):
    ext = (left.at[0], right.at[0])

    @pl.loop(0, ky, unroll=8)
    def _(y):
        part = dot(ex[...], stack3(load_rows(ext, y, kx, ky)))
        store_rows(tmp, y * kx, kx, part)

    @pl.loop(0, kx, unroll=8)
    def _(p):
        part = dot(ey[...], stack3(load_rows(tmp, p, ky, kx)))
        out[0, pl.ds(pl.multiple_of(p * ky, 8), ky), :] = part

    @pl.when(pl.program_id(1) == 0)
    def _():
        edge[0] = out[0, :, :LANES]

    @pl.when(pl.program_id(1) == pl.num_programs(1) - 1)
    def _():
        lane = lax.broadcasted_iota(jnp.int32, edge.shape[1:], 1)
        edge[0] = jnp.where(lane < LANES // 2, edge[0], out[0, :, LANES:])


def forward_xy(ext, ex3, ey3, kx, ky):
    nv, rows, mz = ext.shape
    wide = 2 * LANES
    return pl.pallas_call(
        functools.partial(forward_kernel, kx, ky),
        grid=(nv, mz // wide),
        out_shape=(
            jax.ShapeDtypeStruct(ext.shape, F32),
            jax.ShapeDtypeStruct((nv, rows, LANES), F32),
        ),
        in_specs=[
            pl.BlockSpec((1, rows, LANES), lambda v, z: (v, 0, 2 * z)),
            pl.BlockSpec((1, rows, LANES), lambda v, z: (v, 0, 2 * z + 1)),
            pl.BlockSpec(memory_space=pltpu.VMEM),
            pl.BlockSpec(memory_space=pltpu.VMEM),
        ],
        out_specs=(
            pl.BlockSpec((1, rows, wide), lambda v, z: (v, 0, z)),
            pl.BlockSpec((1, rows, LANES), lambda v, z: (v, 0, 0)),
        ),
        scratch_shapes=[pltpu.VMEM((rows, LANES), F32)] * 2,
        compiler_params=pltpu.CompilerParams(vmem_limit_bytes=56 * 2**20),
        name="forward_xy",
    )(ext, ext, ex3, ey3)


def z_kernel(mz, t, low, high, lxy, lz, w1, w2, out):
    w = NODES
    lane = lax.broadcasted_iota(jnp.int32, low.shape, 1)
    edge = jnp.where(lane < w, high[...], jnp.where(lane >= LANES - w, low[...], 0.0))

    def pack(x):
        hi = x.astype(BF).astype(F32)
        lo = x - hi
        return (hi + pltpu.roll(lo, 2 * w, 1) + pltpu.roll(hi, 4 * w, 1)).astype(BF)

    hi, lo = split(t[...])
    spec = dot(jnp.concatenate([hi, lo, hi, pack(edge)], axis=1), w1[...])
    spec = spec / (lxy[:, :1] + lz[...])
    hi, lo = split(spec[:, :mz])
    out[...] = dot(jnp.concatenate([hi, lo, hi, pack(spec[:, mz:])], axis=1), w2[...])


def solve_z(t, low, high, lxy, lz, w1, w2):
    rows, mz = t.shape
    r = 288
    per = lxy.shape[0] // r
    row = lambda i: (i, 0)
    return pl.pallas_call(
        functools.partial(z_kernel, mz),
        grid=(rows // r,),
        out_shape=jax.ShapeDtypeStruct(t.shape, F32),
        in_specs=[
            pl.BlockSpec((r, mz), row),
            pl.BlockSpec((r, LANES), row),
            pl.BlockSpec((r, LANES), row),
            pl.BlockSpec((r, LANES), lambda i: (lax.rem(i, per), 0)),
            pl.BlockSpec(memory_space=pltpu.VMEM),
            pl.BlockSpec(memory_space=pltpu.VMEM),
            pl.BlockSpec(memory_space=pltpu.VMEM),
        ],
        out_specs=pl.BlockSpec((r, mz), row),
        compiler_params=pltpu.CompilerParams(vmem_limit_bytes=56 * 2**20),
        name="solve_z",
    )(t, low, high, lxy, lz, w1, w2)


def backward_kernel(kx, ky, mx, my, left, right, c3, ex, ey, out, *tmp):
    u = (left.at[0], right.at[0])

    @pl.loop(0, ky, unroll=8)
    def _(q):
        part = dot(ex[...], stack3(load_rows(u, q, kx, ky)))
        store_rows(tmp, q * mx, mx, part)

    @pl.loop(0, mx, unroll=8)
    def _(a):
        slab = stack3(load_rows(tmp, a, ky, mx))
        slab = jnp.concatenate([slab, c3[0, a]], axis=0)
        out[0, pl.ds(pl.multiple_of(a * my, 8), my), :] = dot(ey[...], slab)


def backward_xy(u, c3, ex3, ey3, kx, ky, mx, my):
    nv, rows, mz = u.shape
    wide = 2 * LANES
    return pl.pallas_call(
        functools.partial(backward_kernel, kx, ky, mx, my),
        grid=(nv, mz // wide),
        out_shape=jax.ShapeDtypeStruct((nv, mx * my, mz), F32),
        in_specs=[
            pl.BlockSpec((1, rows, LANES), lambda v, z: (v, 0, 2 * z)),
            pl.BlockSpec((1, rows, LANES), lambda v, z: (v, 0, 2 * z + 1)),
            pl.BlockSpec((1,) + c3.shape[1:3] + (wide,), lambda v, z: (v, 0, 0, z)),
            pl.BlockSpec(memory_space=pltpu.VMEM),
            pl.BlockSpec(memory_space=pltpu.VMEM),
        ],
        out_specs=pl.BlockSpec((1, mx * my, wide), lambda v, z: (v, 0, z)),
        scratch_shapes=[pltpu.VMEM((ky * mx, LANES), F32)] * 2,
        compiler_params=pltpu.CompilerParams(vmem_limit_bytes=56 * 2**20),
        name="backward_xy",
    )(u, u, c3, ex3, ey3)


def left3(m):
    hi, lo = split_host(m)
    return jnp.concatenate([hi, hi, lo], axis=1)


def shifted(x, axis, step):
    count = lax.axis_size(axis)
    pairs = [(i, i + step) for i in range(count) if 0 <= i + step < count]
    return lax.ppermute(x, axis, pairs)


def body(
    residual, eig_x, eig_y, eig_z, lam_x, lam_y, lam_z, basis_x, basis_y, basis_z, coarse_inverse
):
    w = NODES
    nv, mx, my, mz = residual.shape
    kx, ky, kz = eig_x.shape[1], eig_y.shape[1], eig_z.shape[1]
    funcs = basis_x.shape[1]
    bx, by, bz = basis_x[0], basis_y[0], basis_z[0]

    block = funcs**3
    bh, bl = split_host(jnp.tile(bz.T, (1, nv * funcs * funcs)))
    kron = (bx[:, None, :, None] * by[None, :, None, :]).reshape(funcs * funcs, mx * my)
    ext, every = extend(residual, jnp.concatenate([bh, bl], axis=1), left3(kron))
    ext = ext.reshape(nv, kx * ky, mz)

    coarse = jnp.swapaxes(every.reshape(-1, nv, block), 1, 2).reshape(-1, nv)
    coarse = lax.optimization_barrier(coarse)
    sol = lax.optimization_barrier(jnp.dot(coarse_inverse, coarse, precision=HIGH)).T.reshape(nv, funcs, funcs, funcs)
    wide = jnp.einsum("vpqs,pa->vaqs", sol, bx, precision=HIGH)
    wide = jnp.einsum("vaqs,sc->vaqc", wide, bz, precision=HIGH)
    hi, lo = split_host(wide)
    pad = -(3 * funcs) % 16
    c3 = jnp.concatenate([hi, lo, hi, jnp.zeros((nv, mx, pad, mz), BF)], axis=2)

    ex, ey, ez = eig_x[0], eig_y[0], eig_z[0]
    t, edge = forward_xy(ext, left3(ex.T), left3(ey.T), kx, ky)
    edge = edge.reshape(-1, LANES)
    low, high = shifted(edge, "gz", 1), shifted(edge, "gz", -1)

    extra = LANES - (kz - mz)
    eh, el = split_host(jnp.pad(ez, ((0, 0), (0, extra))))
    gap = jnp.zeros((LANES - 7 * w, mz + LANES), BF)
    top, end = slice(0, w), slice(kz - w, kz)
    w1 = jnp.concatenate(
        [eh[w : w + mz], eh[w : w + mz], el[w : w + mz],
         eh[end], eh[top], eh[end], el[top], el[end], gap, jnp.zeros((w, mz + LANES), BF), eh[top]], axis=0)
    bh, bl = split_host(ez[w : w + mz].T)
    gap = jnp.zeros((LANES - 3 * (kz - mz), mz), BF)
    w2 = jnp.concatenate([bh[:mz], bh[:mz], bl[:mz], bh[mz:], bh[mz:], bl[mz:], gap], axis=0)
    lxy = jnp.broadcast_to(
        (lam_x[0][:, None] + lam_y[0][None, :]).reshape(kx * ky, 1), (kx * ky, LANES))
    lz = jnp.pad(lam_z[0], (0, extra), constant_values=1.0)[None]
    u = solve_z(t.reshape(nv * kx * ky, mz), low, high, lxy, lz, w1, w2)

    bh, bl = split_host(by.T)
    ey3 = jnp.concatenate(
        [left3(ey[w : w + my]), bh, bh, bl, jnp.zeros((my, pad), BF)], axis=1)
    out = backward_xy(
        u.reshape(nv, kx * ky, mz), c3, left3(ex[w : w + mx]), ey3, kx, ky, mx, my)
    return out.reshape(nv, mx, my, mz)


def solution(mesh):
    in_specs = (
        P(None, "gx", "gy", "gz"),
        P("gx", None, None),
        P("gy", None, None),
        P("gz", None, None),
        P("gx", None),
        P("gy", None),
        P("gz", None),
        P("gx", None, None),
        P("gy", None, None),
        P("gz", None, None),
        P(("gx", "gy", "gz"), None),
    )
    out_specs = P(None, "gx", "gy", "gz")
    return jax.shard_map(body, mesh=mesh, in_specs=in_specs, out_specs=out_specs, check_vma=False)
```
